256 devices in a mesh: row: 32 (over z, x_hi, core), col: 8 (over x_lo, y).
Axes of the slice: x: 4 (x_hi: 2, x_lo: 2; x = x_hi * 2 + x_lo), y: 4, z: 8, core: 2. Of those that a mesh axis runs over, the one named last changes fastest.
Arguments:
- counts: int32 [16384, 32768], P('row', 'col'), may hold values from 0 to 63
- row_support: int32 [16384], P(('row', 'col')), may hold values from 1 to 2209
- col_support: int32 [32768], P(('col', 'row')), may hold values from 1 to 2209
- total: int32 [1], replicated, may hold values from 256 to 4095
- sketch: bfloat16 [32768, 256], P('col'), may hold values from -6 to 6
Outputs:
- left_basis: float32 [16384, 256], P('row')
- right_basis: float32 [32768, 256], P('col')
The draws below stay inside these ranges and needn't reach their ends.
All inputs are finite; a program needn't handle non-finite values.
Results may differ from the reference program's by a relative error of at most 0.012.
Values may be sent and summed in bfloat16 or wider, within the bound.
No kernel may reach another device: no remote copies, remote signals or barrier semaphores. Data moves between devices by JAX's collectives and lax.ppermute only.
A program may use at most 128 MiB of HBM per device.

```python
import jax
import jax.numpy as jnp
from jax import lax

N = 32768
K = 256
RB_DEV = 512
ROWS = 16384
N_ROW = 32


def support_values(key, length):
    first = jax.random.randint(jax.random.fold_in(key, 11), (length,), 1, 48)
    second = jax.random.randint(jax.random.fold_in(key, 23), (length,), 1, 48)
    return (first * second).astype(jnp.int32)


def draw_row_support(key, part):
    return support_values(jax.random.fold_in(key, 5), ROWS)


def draw_col_support(key, part):
    return support_values(jax.random.fold_in(key, 7), N)


def touch_ends(values, own_key, smallest, high):
    extent = values.shape
    index_at = [jax.random.randint(jax.random.fold_in(own_key, axis), (), 0, extent[axis]) for axis in range(len(extent))]
    values = values.at[tuple(index_at)].set(smallest)
    longest = extent.index(max(extent))
    index_at[longest] = (index_at[longest] + 1) % extent[longest]
    return values.at[tuple(index_at)].set(high)


def block_scale(own_key, extent, shards, low, top_value):
    def one(dim, blocks):
        draws = jax.random.uniform(jax.random.fold_in(jax.random.fold_in(own_key, 6), dim), (blocks,), jnp.float32, low / len(shards), top_value / len(shards))
        return jnp.repeat(jnp.exp(draws), extent[dim] // blocks).reshape((-1,) + (1,) * (len(extent) - dim - 1))

    loudness = one(*shards[0])
    for cut in shards[1:]:
        loudness = loudness * one(*cut)
    return loudness


def centred(own_key, dims, spread, most, shards=(), kind=jnp.bfloat16):
    values = spread * jax.random.normal(own_key, dims, jnp.float32)
    if shards:
        values = values * block_scale(own_key, dims, shards, -0.22, 0.18)
    return jnp.clip(values, -most, most).astype(kind)


def setup_inputs(seed: int = 0) -> dict:
    splits = jax.random.split(jax.random.key(seed), 6)
    return {
        "counts": touch_ends(jax.random.randint(splits[0], (ROWS, N), 0, 64), jax.random.fold_in(splits[0], 1), 0, 63).astype(jnp.int32),
        "row_support": draw_row_support(jax.random.fold_in(splits[5], 71), 0),
        "col_support": draw_col_support(jax.random.fold_in(splits[5], 71), 0),
        "total": jax.random.randint(splits[3], (1,), 256, 4096).astype(jnp.int32),
        "sketch": centred(splits[4], (N, K), 1.0, 6.0, ((0, 8),)),
    }


def lift(block, row_part, col_support, total):
    value = jnp.log(jnp.maximum(block, 1).astype(jnp.float32))
    value = value + jnp.log(total[0].astype(jnp.float32))
    value = value - jnp.log(row_part.astype(jnp.float32))[:, None]
    value = value - jnp.log(col_support.astype(jnp.float32))[None, :]
    return jnp.where(block > 0, jnp.maximum(value, 0.0), 0.0).astype(jnp.bfloat16)

def orthonormal(matrix):
    gram = jnp.dot(matrix.T, matrix, precision=lax.Precision.HIGHEST)
    lower = jnp.linalg.cholesky(gram)
    return jax.scipy.linalg.solve_triangular(lower, matrix.T, lower=True).T

def reference(counts, row_support, col_support, total, sketch):
    blocks = counts.reshape(N_ROW, RB_DEV, N)
    supports = row_support.reshape(N_ROW, RB_DEV)

    def apply_right(rhs):

        def one(pair):
            table = lift(pair[0], pair[1], col_support, total)
            return jnp.dot(table.astype(jnp.float32), rhs.astype(jnp.float32), preferred_element_type=jnp.float32)
        return lax.map(one, (blocks, supports)).reshape(ROWS, K)

    def apply_left(lhs):
        lhs_blocks = lhs.reshape(N_ROW, RB_DEV, K)

        def step(carry, trio):
            table = lift(trio[0], trio[1], col_support, total)
            part = lax.dot_general(table.astype(jnp.float32), trio[2].astype(jnp.float32), (((0,), (0,)), ((), ())), preferred_element_type=jnp.float32)
            return (carry + part, None)
        start = jnp.zeros((N, K), jnp.float32)
        result, _ = lax.scan(step, start, (blocks, supports, lhs_blocks))
        return result
    q_first = orthonormal(apply_right(sketch)).astype(jnp.bfloat16)
    q_second = orthonormal(apply_left(q_first))
    q_third = orthonormal(apply_right(q_second.astype(jnp.bfloat16)))
    return (q_third * jnp.sqrt(jnp.float32(ROWS)), q_second * jnp.sqrt(jnp.float32(N)))
```

```python
import functools

import jax
import jax.numpy as jnp
from jax import lax
from jax.experimental import pallas as pl
from jax.experimental.pallas import tpu as pltpu
from jax.sharding import Mesh
from jax.sharding import PartitionSpec as P

PLANE = ("z", "far")
ROW = ("z", "far", "core")
F32 = jnp.float32
BF16 = jnp.bfloat16
EXACT = lax.Precision.HIGHEST
LEAD = 16
BLOCK = 32


def call(body, out_shape, *args, **options):
    return pl.pallas_call(
        body,
        out_shape=out_shape,
        compiler_params=pltpu.CompilerParams(vmem_limit_bytes=options.pop("vmem", 24) << 20),
        **options,
    )(*args)


def shaped(shape, dtype=F32):
    return jax.ShapeDtypeStruct(shape, dtype)


def exchange(parts, axes):
    return lax.all_to_all(parts, axes, 0, 0, tiled=True)


def copy_for_each(shard, axes):
    count = lax.axis_size(axes)
    return exchange(jnp.broadcast_to(shard[None], (count, *shard.shape)), axes)


def over_rows(left, right, precision=None):
    return lax.dot_general(
        left, right, (((0,), (0,)), ((), ())), precision=precision, preferred_element_type=F32
    )


def over_lanes(left, right, precision=None):
    return lax.dot_general(
        left, right, (((1,), (1,)), ((), ())), precision=precision, preferred_element_type=F32
    )


def lift_body(counts, rows, cols, total, sketch, table, part, acc):
    step = pl.program_id(0)
    base = jnp.log(total[...].astype(F32)) - jnp.log(rows[...].astype(F32))
    block = counts[...]
    value = jnp.log(jnp.maximum(block, 1).astype(F32))
    value = value + base
    value = value - jnp.log(cols[...].astype(F32))
    lifted = jnp.where(block > 0, jnp.maximum(value, 0.0), 0.0).astype(BF16)
    table[...] = lifted
    added = jnp.dot(lifted, sketch[...], preferred_element_type=F32)

    @pl.when(step == 0)
    def _():
        acc[...] = added

    @pl.when(step > 0)
    def _():
        acc[...] += added

    @pl.when(step == pl.num_programs(0) - 1)
    def _():
        part[...] = acc[...]


def lift(counts, rows, cols, total, sketch, wide=512):
    height, width = counts.shape
    rank = sketch.shape[1]
    return call(
        lift_body,
        (shaped((height, width), BF16), shaped((height, rank))),
        counts,
        rows.reshape(height, 1),
        cols.reshape(1, width),
        total.reshape(1, 1),
        sketch,
        grid=(width // wide,),
        in_specs=[
            pl.BlockSpec((height, wide), lambda i: (0, i)),
            pl.BlockSpec((height, 1), lambda i: (0, 0)),
            pl.BlockSpec((1, wide), lambda i: (0, i)),
            pl.BlockSpec((1, 1), lambda i: (0, 0)),
            pl.BlockSpec((wide, rank), lambda i: (i, 0)),
        ],
        out_specs=[
            pl.BlockSpec((height, wide), lambda i: (0, i)),
            pl.BlockSpec((height, rank), lambda i: (0, 0)),
        ],
        scratch_shapes=[pltpu.VMEM((height, rank), F32)],
    )


def summed(ref):
    value = ref[0].astype(F32)
    for i in range(1, ref.shape[0]):
        value = value + ref[i].astype(F32)
    return value


def spread_body(parts, out):
    value = summed(parts)
    for i in range(out.shape[0]):
        out[i] = value


def sum_and_spread(parts, count):
    return call(spread_body, shaped((count, *parts.shape[1:])), parts)


def diag_inverse(tile, lane0, size):
    groups = size // 8
    sub = lax.broadcasted_iota(jnp.int32, (8, 128), 0)
    lane = lax.broadcasted_iota(jnp.int32, (8, 128), 1)
    col = [
        {
            g: jnp.broadcast_to(tile[8 * g : 8 * g + 8, lane0 + j : lane0 + j + 1], (8, 128))
            for g in range(j // 8, groups)
        }
        for j in range(size)
    ]
    inv = [jnp.where(lane == sub + (lane0 + 8 * g), 1.0, 0.0).astype(F32) for g in range(groups)]
    scale = [jnp.zeros((8, 128), F32) for _ in range(groups)]

    def row(value, i):
        return jnp.broadcast_to(value[i : i + 1, :], (8, 128))

    for j in range(size):
        gj, sj = divmod(j, 8)
        root = lax.rsqrt(row(col[j][gj], sj))
        scale[gj] = jnp.where(sub == sj, root, scale[gj])
        over = root * root
        part = {g: col[j][g] * over for g in range(gj, groups)}
        part[gj] = jnp.where(sub > sj, part[gj], 0.0)
        for k in range(j + 1, size):
            pivot = row(col[j][k // 8], k % 8)
            for g in range(k // 8, groups):
                col[k][g] = col[k][g] - part[g] * pivot
        own = row(inv[gj], sj)
        for g in range(gj, groups):
            inv[g] = inv[g] - part[g] * own
    return jnp.concatenate([inv[g] * scale[g] for g in range(groups)], axis=0)


def invert_factor(m, size=BLOCK):
    n = m.shape[0]
    for r0 in range(0, n, size):
        t0 = r0 // 128 * 128
        inv = diag_inverse(m[r0 : r0 + size, t0 : t0 + 128], r0 - t0, size)
        rows = jnp.dot(inv, m[t0 : t0 + 128, :], precision=EXACT, preferred_element_type=F32)
        column = lax.broadcasted_iota(jnp.int32, (size, n), 1)
        wide = jnp.concatenate([inv if t == t0 else jnp.zeros_like(inv) for t in range(0, n, 128)], axis=1)
        done = jnp.where((column >= r0) & (column < r0 + size), wide, rows)
        m[r0 : r0 + size, :] = done
        if r0 + size < n:
            base = (r0 + size) // 128 * 128
            left = jnp.where(column >= r0 + size, rows, 0.0)[:, base:]
            change = over_rows(left, done, EXACT)
            below = m[r0 + size :, :]
            at = lax.broadcasted_iota(jnp.int32, below.shape, 1)
            below = jnp.where((at >= r0) & (at < r0 + size), 0.0, below)
            m[r0 + size :, :] = below - change[r0 + size - base :, :]
    i = lax.broadcasted_iota(jnp.int32, (n, n), 0)
    j = lax.broadcasted_iota(jnp.int32, (n, n), 1)
    return jnp.where(i >= j, m[...], 0.0)


def lead_change(gram):
    lead, rank = gram.shape
    inv = diag_inverse(gram[:, :128], 0, lead)[:, :lead]
    solved = over_rows(inv, jnp.dot(inv, gram, precision=EXACT, preferred_element_type=F32), EXACT)
    i = lax.broadcasted_iota(jnp.int32, (lead, rank), 0)
    j = lax.broadcasted_iota(jnp.int32, (lead, rank), 1)
    unit = jnp.where(i == j, 1.0, 0.0)
    size = jnp.sqrt(jnp.sum(jnp.sum(gram * unit, axis=1, keepdims=True), axis=0, keepdims=True) / lead)
    own = over_rows(inv, unit, EXACT) * size - unit
    return jnp.where(j < lead, own, -solved)


def lead_out(value, change):
    lead = change.shape[0]
    return value + jnp.dot(value[:, :lead], change, precision=EXACT, preferred_element_type=F32)


def lead_gram(value):
    return over_rows(value[:, :128], value, EXACT)[:LEAD, :]


def first_gram_body(value, out):
    gram = lead_gram(value[...])
    for i in range(out.shape[0]):
        out[i] = gram


def send_half_body(core, grams, value, table, first, out):
    cleared = lead_out(value[...], lead_change(summed(grams))).astype(BF16)
    first[...] = cleared
    half = out.shape[0]
    other = pl.multiple_of((1 - core[0]) * half, half)
    out[...] = over_rows(table[:, pl.ds(other, half)], cleared)


def keep_half_body(core, first, table, out):
    half = out.shape[0]
    mine = pl.multiple_of(core[0] * half, half)
    out[...] = over_rows(table[:, pl.ds(mine, half)], first[...])


def add_body(left, right, out):
    out[...] = (left[...] + right[...]).astype(BF16)


def second_gram_body(parts, piece, out):
    value = summed(parts)
    piece[...] = value
    gram = lead_gram(value)
    for i in range(out.shape[0]):
        out[i] = gram


def clear_body(grams, piece, out):
    value = lead_out(piece[...], lead_change(summed(grams))).astype(BF16)
    for i in range(out.shape[0]):
        out[i] = value


def third_body(core, mine, other, table, out):
    half = mine.shape[0]
    at = pl.multiple_of(core[0] * half, half)
    rest = pl.multiple_of((1 - core[0]) * half, half)
    own, far = mine[...], other[...]
    value = jnp.dot(table[:, pl.ds(at, half)], own, preferred_element_type=F32)
    value = value + jnp.dot(table[:, pl.ds(rest, half)], far, preferred_element_type=F32)
    gram = over_rows(own, own) + over_rows(far, far)
    count = out.shape[0]
    deep, thin = value.shape[0] // count, gram.shape[0] // count
    for i in range(count):
        out[i, :deep, :] = value[i * deep : (i + 1) * deep, :]
        out[i, deep:, :] = gram[i * thin : (i + 1) * thin, :]


def third_gram_body(value, out):
    out[...] = over_rows(value[...], value[...], EXACT)


def split(value):
    high = value.astype(BF16)
    return high, (value - high.astype(F32)).astype(BF16)


def last_body(root_left, root_right, core, second, third, mine, other, value, left, right, work, work2):
    work[...] = third[...]
    work2[...] = second[...]
    inverse = invert_factor(work2)
    high, low = split(inverse * root_right)
    half = mine.shape[0]
    for source, at in ((mine, core[0]), (other, 1 - core[0])):
        start = pl.multiple_of(at * half, half)
        right[pl.ds(start, half), :] = over_lanes(source[...], high) + over_lanes(source[...], low)
    left[...] = over_lanes(value[...], invert_factor(work) * root_left, EXACT)


VM = pl.BlockSpec(memory_space=pltpu.VMEM)
SM = pl.BlockSpec(memory_space=pltpu.SMEM)


def per_device(counts, row_support, col_support, total, sketch):
    rows, cols, planes = lax.axis_size(ROW), lax.axis_size("col"), lax.axis_size(PLANE)
    core = lax.axis_index("core").reshape(1).astype(jnp.int32)
    swap = [(0, 1), (1, 0)]
    height, width = counts.shape
    rank = sketch.shape[1]
    half = width // 2

    row_local = copy_for_each(row_support, "col").reshape(-1)
    col_local = copy_for_each(col_support, ROW).reshape(-1)
    table, part = lift(counts, row_local, col_local, total, sketch)

    arrived = exchange(part.reshape(cols, -1, rank), "col")
    first = exchange(sum_and_spread(arrived, cols), "col").reshape(height, rank)
    grams = exchange(call(first_gram_body, shaped((rows, LEAD, rank)), first), ROW)
    cleared, sent = call(
        send_half_body,
        (shaped((height, rank), BF16), shaped((half, rank))),
        core,
        grams,
        first,
        table,
        in_specs=[SM, VM, VM, VM],
        vmem=40,
    )
    got = lax.ppermute(sent, "core", swap)
    kept = call(keep_half_body, shaped((half, rank)), core, cleared, table, in_specs=[SM, VM, VM], vmem=40)
    both = call(add_body, shaped((half, rank), BF16), kept, got)

    parts = exchange(both.reshape(planes, -1, rank), PLANE)
    piece, grams = call(
        second_gram_body, (shaped(parts.shape[1:]), shaped((rows, LEAD, rank))), parts
    )
    grams = exchange(sum_and_spread(exchange(grams, ROW), cols), "col")
    mine = call(clear_body, shaped(parts.shape, BF16), grams, piece)
    mine = exchange(mine, PLANE).reshape(half, rank)
    other = lax.ppermute(mine, "core", swap)

    packed = call(
        third_body,
        shaped((cols, height // cols + rank // cols, rank)),
        core,
        mine,
        other,
        table,
        in_specs=[SM, VM, VM, VM],
        vmem=40,
    )
    packed = exchange(sum_and_spread(exchange(packed, "col"), cols), "col")
    value = packed[:, : height // cols].reshape(height, rank)
    second = packed[:, height // cols :].reshape(rank, rank)
    gram = call(third_gram_body, shaped((rank, rank)), value)
    gram = exchange(sum_and_spread(exchange(gram.reshape(rows, -1, rank), ROW), rows), ROW)
    return tuple(
        call(
            functools.partial(last_body, float(height * rows) ** 0.5, float(width * cols) ** 0.5),
            (shaped((height, rank)), shaped((width, rank))),
            core,
            second,
            gram.reshape(rank, rank),
            mine,
            other,
            value,
            in_specs=[SM, VM, VM, VM, VM, VM],
            scratch_shapes=[pltpu.VMEM((rank, rank), F32), pltpu.VMEM((rank, rank), F32)],
            vmem=40,
        )
    )


def solution(mesh):
    grid = Mesh(mesh.devices.reshape(8, 2, 2, mesh.shape["col"]), ("z", "far", "core", "col"))
    in_specs = (P(ROW, "col"), P((*ROW, "col")), P(("col", *ROW)), P(), P("col", None))
    out_specs = (P(ROW, None), P("col", None))
    return jax.shard_map(per_device, mesh=grid, in_specs=in_specs, out_specs=out_specs, check_vma=False)
```

```python
import functools

import jax
import jax.numpy as jnp
from jax import lax
from jax.experimental import pallas as pl
from jax.experimental.pallas import tpu as pltpu
from jax.sharding import Mesh
from jax.sharding import PartitionSpec as P

PLANE = ("z", "far")
ROW = ("z", "far", "core")
F32 = jnp.float32
BF16 = jnp.bfloat16
EXACT = lax.Precision.HIGHEST
LEAD = 16
FEW = 8
ABSENT = -1e30
RIDGE = 1e-6
TINY = 1e-20
BLOCK = 32


def call(body, out_shape, *args, **options):
    return pl.pallas_call(
        body,
        out_shape=out_shape,
        compiler_params=pltpu.CompilerParams(vmem_limit_bytes=options.pop("vmem", 12) << 20),
        **options,
    )(*args)


def shaped(shape, dtype=F32):
    return jax.ShapeDtypeStruct(shape, dtype)


def in_hbm(value):
    return pltpu.with_memory_space_constraint(value, pltpu.HBM)


def exchange(parts, axes):
    return lax.all_to_all(parts, axes, 0, 0, tiled=True)


def copy_for_each(shard, axes):
    count = lax.axis_size(axes)
    return exchange(jnp.broadcast_to(shard[None], (count, *shard.shape)), axes)


def over_rows(left, right, precision=None):
    return lax.dot_general(
        left, right, (((0,), (0,)), ((), ())), precision=precision, preferred_element_type=F32
    )


def over_lanes(left, right, precision=None):
    return lax.dot_general(
        left, right, (((1,), (1,)), ((), ())), precision=precision, preferred_element_type=F32
    )


def log_body(counts, total, out):
    block = counts[...]
    value = jnp.log(jnp.maximum(block, 1).astype(F32)) + jnp.log(total[...].astype(F32))
    out[...] = jnp.where(block > 0, value, ABSENT)


def logs_of(counts, total, wide=512):
    height, width = counts.shape
    return call(
        log_body,
        pltpu.HBM((height, width), F32),
        in_hbm(counts),
        total.reshape(1, 1),
        grid=(width // wide,),
        in_specs=[pl.BlockSpec((height, wide), lambda i: (0, i)), pl.BlockSpec((1, 1), lambda i: (0, 0))],
        out_specs=pl.BlockSpec((height, wide), lambda i: (0, i)),
        vmem=12,
    )


def lift_body(logs, rows, cols, sketch, table, part, acc):
    step = pl.program_id(0)
    value = logs[...] - jnp.log(rows[...].astype(F32)) - jnp.log(cols[...].astype(F32))
    lifted = jnp.maximum(value, 0.0).astype(BF16)
    table[...] = lifted
    added = jnp.dot(lifted, sketch[...], preferred_element_type=F32)

    @pl.when(step == 0)
    def _():
        acc[...] = added

    @pl.when(step > 0)
    def _():
        acc[...] += added

    @pl.when(step == pl.num_programs(0) - 1)
    def _():
        part[...] = acc[...]


def lift(logs, rows, cols, sketch, wide=512):
    height, width = logs.shape
    rank = sketch.shape[1]
    return call(
        lift_body,
        (pltpu.HBM((height, width), BF16), shaped((height, rank))),
        in_hbm(logs),
        rows.reshape(height, 1),
        cols.reshape(1, width),
        sketch,
        grid=(width // wide,),
        in_specs=[
            pl.BlockSpec((height, wide), lambda i: (0, i)),
            pl.BlockSpec((height, 1), lambda i: (0, 0)),
            pl.BlockSpec((1, wide), lambda i: (0, i)),
            pl.BlockSpec((wide, rank), lambda i: (i, 0)),
        ],
        out_specs=[
            pl.BlockSpec((height, wide), lambda i: (0, i)),
            pl.BlockSpec((height, rank), lambda i: (0, 0)),
        ],
        scratch_shapes=[pltpu.VMEM((height, rank), F32)],
        vmem=12,
    )


def summed(ref):
    value = ref[0].astype(F32)
    for i in range(1, ref.shape[0]):
        value = value + ref[i].astype(F32)
    return value


def spread_body(parts, out):
    value = summed(parts)
    for i in range(out.shape[0]):
        out[i] = value


def sum_and_spread(parts, count):
    return call(spread_body, shaped((count, *parts.shape[1:])), parts)


def diag_inverse(tile, lane0, size):
    groups = size // 8
    sub = lax.broadcasted_iota(jnp.int32, (8, 128), 0)
    lane = lax.broadcasted_iota(jnp.int32, (8, 128), 1)
    col = [
        {
            g: jnp.broadcast_to(tile[8 * g : 8 * g + 8, lane0 + j : lane0 + j + 1], (8, 128))
            for g in range(j // 8, groups)
        }
        for j in range(size)
    ]
    inv = [jnp.where(lane == sub + (lane0 + 8 * g), 1.0, 0.0).astype(F32) for g in range(groups)]
    scale = [jnp.zeros((8, 128), F32) for _ in range(groups)]

    def row(value, i):
        return jnp.broadcast_to(value[i : i + 1, :], (8, 128))

    for j in range(size):
        gj, sj = divmod(j, 8)
        root = lax.rsqrt(row(col[j][gj], sj))
        scale[gj] = jnp.where(sub == sj, root, scale[gj])
        over = root * root
        part = {g: col[j][g] * over for g in range(gj, groups)}
        part[gj] = jnp.where(sub > sj, part[gj], 0.0)
        for k in range(j + 1, size):
            pivot = row(col[j][k // 8], k % 8)
            for g in range(k // 8, groups):
                col[k][g] = col[k][g] - part[g] * pivot
        own = row(inv[gj], sj)
        for g in range(gj, groups):
            inv[g] = inv[g] - part[g] * own
    return jnp.concatenate([inv[g] * scale[g] for g in range(groups)], axis=0)


def invert_factor(m, size=BLOCK):
    n = m.shape[0]
    for r0 in range(0, n, size):
        t0 = r0 // 128 * 128
        inv = diag_inverse(m[r0 : r0 + size, t0 : t0 + 128], r0 - t0, size)
        rows = jnp.dot(inv, m[t0 : t0 + 128, :], precision=EXACT, preferred_element_type=F32)
        column = lax.broadcasted_iota(jnp.int32, (size, n), 1)
        wide = jnp.concatenate([inv if t == t0 else jnp.zeros_like(inv) for t in range(0, n, 128)], axis=1)
        done = jnp.where((column >= r0) & (column < r0 + size), wide, rows)
        m[r0 : r0 + size, :] = done
        if r0 + size < n:
            base = (r0 + size) // 128 * 128
            left = jnp.where(column >= r0 + size, rows, 0.0)[:, base:]
            change = over_rows(left, done, EXACT)
            below = m[r0 + size :, :]
            at = lax.broadcasted_iota(jnp.int32, below.shape, 1)
            below = jnp.where((at >= r0) & (at < r0 + size), 0.0, below)
            m[r0 + size :, :] = below - change[r0 + size - base :, :]
    i = lax.broadcasted_iota(jnp.int32, (n, n), 0)
    j = lax.broadcasted_iota(jnp.int32, (n, n), 1)
    return jnp.where(i >= j, m[...], 0.0)


def lead_rows(gram):
    lead, rank = gram.shape
    i = lax.broadcasted_iota(jnp.int32, (lead, rank), 0)
    j = lax.broadcasted_iota(jnp.int32, (lead, rank), 1)
    size = jnp.sum(jnp.sum(jnp.where(i == j, gram, 0.0), axis=1, keepdims=True), axis=0, keepdims=True)
    gram = gram + jnp.where(i == j, size * RIDGE + TINY, 0.0)
    inv = diag_inverse(gram[:, :128], 0, lead)[:, :lead]
    solved = over_rows(inv, jnp.dot(inv, gram, precision=EXACT, preferred_element_type=F32), EXACT)
    return inv, solved, jnp.where(i == j, 1.0, 0.0), j < lead, size


def lead_change(gram):
    inv, solved, unit, lead, size = lead_rows(gram)
    own = over_rows(inv, unit, EXACT) * jnp.sqrt(size / gram.shape[0]) - unit
    return jnp.where(lead, own, -solved)


def lead_out(value, change):
    lead = change.shape[0]
    return value + jnp.dot(value[:, :lead], change, precision=EXACT, preferred_element_type=F32)


def split(value):
    high = value.astype(BF16)
    return high, (value - high.astype(F32)).astype(BF16)


def half_body(core, value, table, out, high, low):
    del core

    @pl.when(pl.program_id(0) == 0)
    def _():
        high[...], low[...] = split(value[...])

    columns = table[...]
    out[...] = over_rows(columns, high[...]) + over_rows(columns, low[...])


def half_product(other, core, value, table, wide=512):
    height, rank = value.shape
    half = table.shape[1] // 2
    steps = half // wide

    def at(i, core):
        return (0, (1 - core[0] if other else core[0]) * steps + i)

    return call(
        half_body,
        shaped((half, rank)),
        core,
        value,
        in_hbm(table),
        grid_spec=pltpu.PrefetchScalarGridSpec(
            num_scalar_prefetch=1,
            grid=(steps,),
            in_specs=[
                pl.BlockSpec((height, rank), lambda i, core: (0, 0)),
                pl.BlockSpec((height, wide), at),
            ],
            out_specs=pl.BlockSpec((wide, rank), lambda i, core: (i, 0)),
            scratch_shapes=[pltpu.VMEM((height, rank), BF16), pltpu.VMEM((height, rank), BF16)],
        ),
    )


def encode(value, out, count):
    tall, rank = value.shape
    deep = tall // count
    inv, solved, unit, lead, size = lead_rows(over_rows(value[:, :128], value, EXACT)[:FEW, :])
    across = jnp.where(lead, unit, solved).astype(BF16).astype(F32)
    lane = lax.broadcasted_iota(jnp.int32, (tall, 128), 1)
    down = jnp.where(lane < FEW, value[:, :128], 0.0).astype(BF16)
    turned = over_lanes(unit[:, :128].astype(BF16), down)
    rest = (value - over_rows(turned, across)).astype(BF16)
    for k in range(out.shape[0]):
        own = k % count * deep
        out[k, :deep, :] = rest[own : own + deep, :]
        tail = jnp.concatenate([turned[:, own : own + deep], jnp.zeros((FEW, rank - deep), F32)], axis=1)
        out[k, deep:, :] = jnp.concatenate([across, tail], axis=0).astype(BF16)


def encode_sum_body(left, right, out):
    encode(left[...] + right[...], out, out.shape[0])


def encode_parts_body(parts, out):
    count, tall, rank = parts.shape
    deep = tall - 2 * FEW
    tails = [parts[k, deep:, :].astype(F32) for k in range(count)]
    down = jnp.concatenate([tail[FEW:, :deep] for tail in tails], axis=0)
    across = jnp.concatenate([tail[:FEW, :] for tail in tails], axis=0)
    value = over_rows(down, across)
    for k in range(count):
        value = value + parts[k, :deep, :].astype(F32)
    encode(value, out, 1)


def decode_body(core, mine, other, value, out):
    count, tall, rank = mine.shape
    deep = tall - 2 * FEW
    for source, at in ((mine, core[0]), (other, 1 - core[0])):
        for k in range(count):
            tail = source[k, deep:, :].astype(F32)
            block = source[k, :deep, :].astype(F32) + over_rows(tail[FEW:, :deep], tail[:FEW, :])
            start = pl.multiple_of(at * (count * deep) + k * deep, deep)
            value[pl.ds(start, deep), :] = block
    total = jnp.zeros((128, rank), F32)
    for start in range(0, value.shape[0], 512):
        block = value[start : start + 512, :]
        total = total + over_rows(block[:, :128], block, EXACT)
    for i in range(out.shape[0]):
        out[i] = total[:LEAD, :]


def third_body(grams, value, table, second, out):
    cleared = lead_out(value[...], lead_change(summed(grams))).astype(BF16)
    second[...] = cleared
    product = jnp.dot(table[...], cleared, preferred_element_type=F32)
    gram = over_rows(cleared, cleared)
    count = out.shape[0]
    deep, thin = product.shape[0] // count, gram.shape[0] // count
    for i in range(count):
        out[i, :deep, :] = product[i * deep : (i + 1) * deep, :]
        out[i, deep:, :] = gram[i * thin : (i + 1) * thin, :]


def unpacked(packed, start, stop):
    return jnp.concatenate([packed[i, start:stop, :] for i in range(packed.shape[0])], axis=0)


def third_gram_body(packed, out):
    value = unpacked(packed, 0, packed.shape[1] - packed.shape[2] // packed.shape[0])
    gram = over_rows(value, value, EXACT)
    thin = out.shape[1]
    for i in range(out.shape[0]):
        out[i] = gram[i * thin : (i + 1) * thin, :]


def right_body(root, packed, second, out, work):
    work[...] = unpacked(packed, packed.shape[1] - packed.shape[2] // packed.shape[0], packed.shape[1])
    high, low = split(invert_factor(work) * root)
    deep = second.shape[0] // 8
    for i in range(8):
        part = second[i * deep : (i + 1) * deep, :]
        out[i * deep : (i + 1) * deep, :] = over_lanes(part, high) + over_lanes(part, low)


def left_body(root, packed, third, out, work):
    work[...] = third[...]
    value = unpacked(packed, 0, packed.shape[1] - packed.shape[2] // packed.shape[0])
    out[...] = over_lanes(value, invert_factor(work) * root, EXACT)


VM = pl.BlockSpec(memory_space=pltpu.VMEM)
SM = pl.BlockSpec(memory_space=pltpu.SMEM)


def per_device(counts, row_support, col_support, total, sketch):
    rows, cols, planes = lax.axis_size(ROW), lax.axis_size("col"), lax.axis_size(PLANE)
    core = lax.axis_index("core").reshape(1).astype(jnp.int32)
    swap = [(0, 1), (1, 0)]
    height, width = counts.shape
    rank = sketch.shape[1]
    half = width // 2

    row_local = copy_for_each(row_support, "col").reshape(-1)
    col_local = copy_for_each(col_support, ROW).reshape(-1)
    logs = logs_of(counts, total)
    table, part = lift(logs, row_local, col_local, sketch)

    arrived = exchange(part.reshape(cols, -1, rank), "col")
    first = exchange(sum_and_spread(arrived, cols), "col").reshape(height, rank)
    sides = [half_product(other, core, first, table) for other in (True, False)]
    got = lax.ppermute(sides[0], "core", swap)
    deep = half // planes
    coded = shaped((planes, deep + 2 * FEW, rank), BF16)
    parts = exchange(call(encode_sum_body, coded, sides[1], got, vmem=16), PLANE)
    mine = call(encode_parts_body, coded, parts, vmem=12)
    mine = exchange(mine, PLANE)
    other = lax.ppermute(mine, "core", swap)
    value, grams = call(
        decode_body,
        (shaped((width, rank)), shaped((cols, LEAD, rank))),
        core,
        mine,
        other,
        in_specs=[SM, VM, VM],
        vmem=20,
    )
    grams = exchange(grams, "col")
    second, packed = call(
        third_body,
        (shaped((width, rank), BF16), shaped((cols, height // cols + rank // cols, rank))),
        grams,
        value,
        table,
        vmem=24,
    )
    packed = exchange(sum_and_spread(exchange(packed, "col"), cols), "col")
    gram = call(third_gram_body, shaped((rows, rank // rows, rank)), packed, vmem=12)
    gram = exchange(sum_and_spread(exchange(gram, ROW), rows), ROW)
    work = [pltpu.VMEM((rank, rank), F32)]
    right = call(
        functools.partial(right_body, float(width * cols) ** 0.5),
        shaped((width, rank)),
        packed,
        second,
        scratch_shapes=work,
        vmem=20,
    )
    left = call(
        functools.partial(left_body, float(height * rows) ** 0.5),
        shaped((height, rank)),
        packed,
        gram.reshape(rank, rank),
        scratch_shapes=work,
        vmem=12,
    )
    return left, right


def solution(mesh):
    grid = Mesh(mesh.devices.reshape(8, 2, 2, mesh.shape["col"]), ("z", "far", "core", "col"))
    in_specs = (P(ROW, "col"), P((*ROW, "col")), P(("col", *ROW)), P(), P("col", None))
    out_specs = (P(ROW, None), P("col", None))
    return jax.shard_map(per_device, mesh=grid, in_specs=in_specs, out_specs=out_specs, check_vma=False)
```
